32 devices in a mesh: dp: 4 (over z), mp: 8 (over y, x, core).
Axes of the slice: x: 2, y: 2, z: 4, core: 2. Of those that a mesh axis runs over, the one named last changes fastest.
Arguments:
- weight: bfloat16 [5120, 32768], P('dp', 'mp'), may hold values from -0.078125 to 0.078125
- rank_map: int32 [8], replicated, may hold values from 0 to 7, each once
Outputs:
- quant_out: bfloat16 [5120, 32768], P(None, 'mp')
- scale_out: bfloat16 [5120, 256], P(None, 'mp')
- checksum: float32 [256], replicated
The draws below stay inside these ranges and needn't reach their ends.
Inputs may be any that keep to these rules, and one draw needn't show every extreme that they name: `rank_map`: a permutation of 0 to 7.
All inputs are finite; a program needn't handle non-finite values.
Results may differ from the reference program's by a relative error of at most 0.0085.
Values may be sent and summed in bfloat16 or wider, within the bound.
A program may use at most 192 MiB of HBM per device.

```python
import math
import jax
import jax.numpy as jnp
from jax import lax

D = 5120
F = 32768
N_MP = 8


def level_of(key, shape, pieces, smallest, largest):
    factor_of = 1.0
    for position, parts in pieces:
        draws = jax.random.uniform(jax.random.fold_in(jax.random.fold_in(key, 6), position), (parts,), jnp.float32, smallest / len(pieces), largest / len(pieces))
        factor_of = factor_of * jnp.repeat(jnp.exp(draws), shape[position] // parts).reshape((-1,) + (1,) * (len(shape) - 1 - position))
    return factor_of


def scatter_about(stream_key, dims, deviation, limit, shards=(), dtype=jnp.bfloat16):
    values = jax.random.normal(stream_key, dims, jnp.float32) * deviation
    if len(shards) > 0:
        values = level_of(stream_key, dims, shards, -0.22, 0.18) * values
    return jnp.clip(values, min=-limit, max=limit).astype(dtype)


def setup_inputs(seed: int = 0) -> dict:
    key_of = jax.random.split(jax.random.key(seed), 3)
    weight = scatter_about(key_of[0], (D, F), D ** -0.5, 0.078125, ((0, 4), (1, 8)))
    rank_map = jax.random.permutation(key_of[1], N_MP).astype(jnp.int32)
    return {"weight": weight, "rank_map": rank_map}


floor_ratio = 0.25

def quantize(weight):
    rows, cols = weight.shape
    blocks = weight.astype(jnp.float32).reshape(rows, cols // 128, 128)
    peak = lax.optimization_barrier(jnp.max(jnp.abs(blocks), axis=2))
    scale = (jnp.maximum(peak, floor_ratio / math.sqrt(D)) / 127.0).astype(jnp.bfloat16)
    quant = (blocks / scale.astype(jnp.float32)[:, :, None]).astype(jnp.bfloat16)
    return (quant, scale)

def inverse(rank_map):
    count = rank_map.shape[0]
    ids = jnp.arange(count).astype(jnp.int32)
    match = (rank_map[None, :] == ids[:, None]).astype(jnp.int32)
    return lax.optimization_barrier(jnp.sum(ids[None, :] * match, axis=1)).astype(jnp.int32)

def reference(weight, rank_map):
    quant, scale = quantize(weight)
    total = lax.optimization_barrier(jnp.sum(quant.astype(jnp.float32), axis=(0, 2)))
    checksum = total / (127.0 * math.sqrt(D * 128))
    inv = inverse(rank_map)
    blocks = F // 128
    local = blocks // N_MP
    order = (jnp.arange(local).astype(jnp.int32)[None, :] * N_MP + inv[:, None]).reshape(-1).astype(jnp.int32)
    quant_out = jnp.take(quant, order, axis=1).reshape(D, F)
    scale_out = jnp.take(scale, order, axis=1)
    return (quant_out, scale_out, checksum)
```

```python
import functools
import math

import jax
import jax.numpy as jnp
from jax import lax
from jax.experimental import pallas as pl
from jax.experimental.pallas import tpu as pltpu
from jax.sharding import PartitionSpec as P

LANES = 128
FLOOR_RATIO = 0.25
CHUNKS = 2
MESH = pl.DeviceIdType.MESH


def inverse(rank_map):
    count = rank_map.shape[0]
    ids = jnp.arange(count, dtype=jnp.int32)
    match = (rank_map[None, :] == ids[:, None]).astype(jnp.int32)
    return jnp.sum(ids[None, :] * match, axis=1).astype(jnp.int32)


def quantize_kernel(floor, count, group, inv_ref, w_ref, q_ref, s_ref, p_ref, acc_ref):
    step = pl.program_id(0)
    tile = w_ref.shape[0]
    nblocks = count * group

    @pl.when(step == 0)
    def _():
        acc_ref[...] = jnp.zeros_like(acc_ref)

    lane = lax.broadcasted_iota(jnp.int32, (tile, LANES), 1)
    scales = jnp.zeros((tile, LANES), jnp.float32)
    for r in range(count):
        for i in range(group):
            b = i * count + inv_ref[r]
            x = w_ref[:, pl.ds(pl.multiple_of(b * LANES, LANES), LANES)].astype(jnp.float32)
            peak = jnp.max(jnp.abs(x), axis=1, keepdims=True)
            scale = (jnp.maximum(peak, floor) / 127.0).astype(jnp.bfloat16).astype(jnp.float32)
            q = (x * (1.0 / scale)).astype(jnp.bfloat16)
            q_ref[r, :, i * LANES:(i + 1) * LANES] = q
            scales = jnp.where(lane == r * group + i, scale, scales)
            acc_ref[pl.ds(b, 1), :] += jnp.sum(q.astype(jnp.float32), axis=0, keepdims=True)
    s_ref[0] = scales.T[:nblocks].astype(jnp.bfloat16)

    @pl.when(step == pl.num_programs(0) - 1)
    def _():
        sums = jnp.sum(acc_ref[...], axis=1, keepdims=True)
        row = lax.broadcasted_iota(jnp.int32, (nblocks, LANES), 0)
        col = lax.broadcasted_iota(jnp.int32, (nblocks, LANES), 1)
        line = jnp.sum(jnp.where(row == col, sums, 0.0), axis=0, keepdims=True)
        p_ref[...] = jnp.broadcast_to(line, p_ref.shape)


def quantize(weight, inv, total_rows):
    rows, cols = weight.shape
    count = inv.shape[0]
    group = cols // LANES // count
    nblocks = count * group
    tile = LANES
    steps = rows // tile
    floor = FLOOR_RATIO / math.sqrt(total_rows)
    return pl.pallas_call(
        functools.partial(quantize_kernel, floor, count, group),
        grid_spec=pltpu.PrefetchScalarGridSpec(
            num_scalar_prefetch=1,
            grid=(steps,),
            in_specs=[pl.BlockSpec((tile, cols), lambda t, inv: (t, 0))],
            out_specs=[
                pl.BlockSpec((count, tile, group * LANES), lambda t, inv: (0, t, 0)),
                pl.BlockSpec((1, nblocks, LANES), lambda t, inv: (t, 0, 0)),
                pl.BlockSpec((8, LANES), lambda t, inv: (0, 0)),
            ],
            scratch_shapes=[pltpu.VMEM((nblocks, LANES), jnp.float32)],
        ),
        out_shape=[
            jax.ShapeDtypeStruct((count, rows, group * LANES), jnp.bfloat16),
            jax.ShapeDtypeStruct((steps, nblocks, LANES), jnp.bfloat16),
            jax.ShapeDtypeStruct((8, LANES), jnp.float32),
        ],
        compiler_params=pltpu.CompilerParams(dimension_semantics=("arbitrary",)),
        cost_estimate=pl.CostEstimate(flops=rows * cols * 8, bytes_accessed=rows * cols * 4, transcendentals=0),
    )(inv, weight)


def flip(m, k):
    bit, out = 1, m
    while bit <= k:
        if k & bit:
            out = out + bit - 2 * bit * ((m // bit) % 2)
        bit *= 2
    return out


def move_kernel(n, count, q_ref, s_ref, p_ref, out_ref, so_ref, po_ref,
                a_send, a_recv, z_send, z_recv, own_sem):
    z = lax.axis_index("dp")
    m = lax.axis_index("mp")
    rows, width = q_ref.shape[1:]
    chunk = rows // CHUNKS
    right, left = (z + 1) % n, (z + n - 1) % n
    near = {1: right, -1: left}
    half = n // 2
    order = sorted(range(1, count), key=lambda k: (bin(k).count("1"), k))

    barrier = pltpu.get_barrier_semaphore()
    for k in range(1, count):
        pl.semaphore_signal(barrier, inc=1, device_id=(z, flip(m, k)), device_id_type=MESH)
    for peer in (right, left):
        pl.semaphore_signal(barrier, inc=1, device_id=(peer, m), device_id_type=MESH)
    pl.semaphore_wait(barrier, count + 1)

    def place(origin, c, src):
        return out_ref.at[pl.ds(pl.multiple_of(origin * rows + c * chunk, 16), chunk),
                          pl.ds(pl.multiple_of(src * width, LANES), width)]

    def plane(unit):
        c, k = unit
        peer = flip(m, k)
        if c < CHUNKS:
            src, dst = q_ref.at[peer, pl.ds(c * chunk, chunk)], place(z, c, m)
        elif c == CHUNKS:
            src, dst = s_ref.at[peer], so_ref.at[z, m]
        else:
            src, dst = p_ref, po_ref.at[z, m]
        return pltpu.make_async_remote_copy(
            src_ref=src, dst_ref=dst, send_sem=a_send.at[c, k - 1], recv_sem=a_recv.at[c, k - 1],
            device_id=(z, peer), device_id_type=MESH)

    def ring(unit, way, hop):
        c, k = unit
        origin = (z + n - way * (hop - 1)) % n
        if c < CHUNKS:
            dst = place(origin, c, flip(m, k))
            src = q_ref.at[m, pl.ds(c * chunk, chunk)] if k == 0 and hop == 1 else dst
        else:
            src = dst = (so_ref if c == CHUNKS else po_ref).at[origin]
        w = 0 if way == 1 else 1
        return pltpu.make_async_remote_copy(
            src_ref=src, dst_ref=dst, send_sem=z_send.at[w, hop - 1, c, k], recv_sem=z_recv.at[w, hop - 1, c, k],
            device_id=(near[way], m), device_id_type=MESH)

    def own(unit):
        c, _ = unit
        if c < CHUNKS:
            src, dst = q_ref.at[m, pl.ds(c * chunk, chunk)], place(z, c, m)
        elif c == CHUNKS:
            src, dst = s_ref.at[m], so_ref.at[z, m]
        else:
            src, dst = p_ref, po_ref.at[z, m]
        return pltpu.make_async_copy(src, dst, own_sem.at[c])

    bulk = [(c, k) for c in range(CHUNKS) for k in [0] + order]
    small = [(CHUNKS, 0), (CHUNKS + 1, 0)]
    units = bulk[:-2] + small + bulk[-2:]
    parity = {unit: j % 2 for j, unit in enumerate(units)}

    def ways(unit, hop):
        if hop < half or n % 2:
            return (1, -1)
        return (1,) if parity[unit] == 0 else (-1,)

    hops = half
    started = []

    def go(copy):
        copy.start()
        started.append(copy)

    for way in ways((0, 0), 1):
        go(ring((0, 0), way, 1))
    for k in order:
        go(plane((0, k)))
    for c in range(1, CHUNKS):
        for way in ways((c, 0), 1):
            go(ring((c, 0), way, 1))
    for c in range(1, CHUNKS + 2):
        for k in order:
            go(plane((c, k)))
    owned = [own((c, 0)) for c in range(CHUNKS + 2)]
    for copy in owned:
        copy.start()

    for unit in units:
        c, k = unit
        if c < CHUNKS and k == 0:
            continue
        if c < CHUNKS:
            plane(unit).wait_recv()
        else:
            owned[c].wait()
            for peer in order:
                plane((c, peer)).wait_recv()
        for way in ways(unit, 1):
            go(ring(unit, way, 1))
    for hop in range(2, hops + 1):
        for unit in units:
            for way in (1, -1):
                if way in ways(unit, hop - 1):
                    if way in ways(unit, hop):
                        ring(unit, way, hop - 1).wait_recv()
                        go(ring(unit, way, hop))
    for hop in range(1, hops + 1):
        for unit in units:
            for way in ways(unit, hop):
                if hop == hops or way not in ways(unit, hop + 1):
                    ring(unit, way, hop).wait_recv()
    for copy in owned[:CHUNKS]:
        copy.wait()
    for copy in started:
        copy.wait_send()


def move(quant, scale, sums, n):
    count, rows, width = quant.shape
    hops = max(n // 2, 1)
    any_spec = pl.BlockSpec(memory_space=pl.ANY)
    dma = pltpu.SemaphoreType.DMA
    sent = rows * width * count * 2 * (n - 1)
    return pl.pallas_call(
        functools.partial(move_kernel, n, count),
        in_specs=[any_spec] * 3,
        out_specs=[any_spec] * 3,
        out_shape=[
            jax.ShapeDtypeStruct((n * rows, count * width), quant.dtype),
            jax.ShapeDtypeStruct((n, count) + scale.shape[1:], scale.dtype),
            jax.ShapeDtypeStruct((n, count) + sums.shape, sums.dtype),
        ],
        scratch_shapes=[
            dma((CHUNKS + 2, count - 1)),
            dma((CHUNKS + 2, count - 1)),
            dma((2, hops, CHUNKS + 2, count)),
            dma((2, hops, CHUNKS + 2, count)),
            dma((CHUNKS + 2,)),
        ],
        compiler_params=pltpu.CompilerParams(collective_id=0, has_side_effects=True),
        cost_estimate=pl.CostEstimate(flops=0, bytes_accessed=sent * 2, transcendentals=0),
    )(quant, scale, sums)


def local(n, weight, rank_map):
    inv = inverse(rank_map)
    rows, cols = weight.shape
    count = rank_map.shape[0]
    group = cols // LANES // count
    nblocks = count * group
    total_rows = rows * n
    quant, scale, sums = quantize(weight, inv, total_rows)
    steps = scale.shape[0]
    scale = scale.reshape(steps, count, group, LANES).transpose(1, 0, 2, 3).reshape(count, steps * group, LANES)
    quant_out, scales, partial_sums = move(quant, scale, sums, n)
    scales = scales.reshape(n, count, steps, group, LANES).transpose(0, 2, 4, 1, 3)
    scale_out = scales.reshape(total_rows, nblocks)
    totals = jnp.sum(partial_sums[:, :, 0, :nblocks], axis=0).reshape(-1)
    return (quant_out, scale_out, totals / (127.0 * math.sqrt(total_rows * LANES)))


def solution(mesh):
    n = mesh.shape["dp"]
    in_specs = (P("dp", "mp"), P())
    out_specs = (P(None, "mp"), P(None, "mp"), P())
    return jax.shard_map(functools.partial(local, n), mesh=mesh, in_specs=in_specs, out_specs=out_specs, check_vma=False)
```

```python
import functools
import math

import jax
import jax.numpy as jnp
from jax import lax
from jax.experimental import pallas as pl
from jax.experimental.pallas import tpu as pltpu
from jax.sharding import PartitionSpec as P


LANES = 128
FLOOR_RATIO = 0.25
CHUNKS = 2
MESH = pl.DeviceIdType.MESH


TAIL_PART = 5


def inverse_of(map_ref, count, r):
    inv = 0
    for j in range(count):
        inv = inv + jnp.where(map_ref[j] == r, j, 0)
    return inv


def scaled(x, floor):
    peak = jnp.max(jnp.abs(x), axis=1, keepdims=True)
    scale = (jnp.maximum(peak, floor) / 127.0).astype(jnp.bfloat16).astype(jnp.float32)
    return (x * (1.0 / scale)).astype(jnp.bfloat16), scale


def head_kernel(floor, map_ref, here_ref, w_ref, q_ref):
    q_ref[...] = scaled(w_ref[...].astype(jnp.float32), floor)[0]


def quantize_head(weight, rank_map, here, floor, main):
    _, cols = weight.shape
    count = rank_map.shape[0]
    group = cols // LANES // count
    return pl.pallas_call(
        functools.partial(head_kernel, floor),
        grid_spec=pltpu.PrefetchScalarGridSpec(
            num_scalar_prefetch=2,
            grid=(group,),
            in_specs=[pl.BlockSpec((main, LANES), lambda i, rm, here: (0, i * count + inverse_of(rm, count, here[1])))],
            out_specs=pl.BlockSpec((main, LANES), lambda i, rm, here: (0, i)),
        ),
        out_shape=jax.ShapeDtypeStruct((main, group * LANES), jnp.bfloat16),
        compiler_params=pltpu.CompilerParams(dimension_semantics=("arbitrary",)),
        cost_estimate=pl.CostEstimate(flops=0, bytes_accessed=main * group * LANES * 4, transcendentals=0),
    )(rank_map, here, weight)


def quantize_kernel(floor, count, group, map_ref, w_ref, q_ref, s_ref, p_ref, acc_ref):
    step = pl.program_id(0)
    tile = w_ref.shape[0]
    nblocks = count * group

    @pl.when(step == 0)
    def _():
        acc_ref[...] = jnp.zeros_like(acc_ref)

    lane = lax.broadcasted_iota(jnp.int32, (tile, LANES), 1)
    scales = jnp.zeros((tile, LANES), jnp.float32)
    for r in range(count):
        inv = inverse_of(map_ref, count, r)
        for i in range(group):
            b = i * count + inv
            x = w_ref[:, pl.ds(pl.multiple_of(b * LANES, LANES), LANES)].astype(jnp.float32)
            q, scale = scaled(x, floor)
            q_ref[r, :, i * LANES:(i + 1) * LANES] = q
            scales = jnp.where(lane == r * group + i, scale, scales)
            acc_ref[pl.ds(b, 1), :] += jnp.sum(q.astype(jnp.float32), axis=0, keepdims=True)
    s_ref[0] = scales.T[:nblocks].astype(jnp.bfloat16)

    @pl.when(step == pl.num_programs(0) - 1)
    def _():
        sums = jnp.sum(acc_ref[...], axis=1, keepdims=True)
        row = lax.broadcasted_iota(jnp.int32, (nblocks, LANES), 0)
        col = lax.broadcasted_iota(jnp.int32, (nblocks, LANES), 1)
        line = jnp.sum(jnp.where(row == col, sums, 0.0), axis=0, keepdims=True)
        p_ref[...] = jnp.broadcast_to(line, p_ref.shape)


def quantize(weight, inv, floor):
    rows, cols = weight.shape
    count = inv.shape[0]
    group = cols // LANES // count
    nblocks = count * group
    tile = LANES
    steps = rows // tile
    return pl.pallas_call(
        functools.partial(quantize_kernel, floor, count, group),
        grid_spec=pltpu.PrefetchScalarGridSpec(
            num_scalar_prefetch=1,
            grid=(steps,),
            in_specs=[pl.BlockSpec((tile, cols), lambda t, inv: (t, 0))],
            out_specs=[
                pl.BlockSpec((count, tile, group * LANES), lambda t, inv: (0, t, 0)),
                pl.BlockSpec((1, nblocks, LANES), lambda t, inv: (t, 0, 0)),
                pl.BlockSpec((8, LANES), lambda t, inv: (0, 0)),
            ],
            scratch_shapes=[pltpu.VMEM((nblocks, LANES), jnp.float32)],
        ),
        out_shape=[
            jax.ShapeDtypeStruct((count, rows, group * LANES), jnp.bfloat16),
            jax.ShapeDtypeStruct((steps, nblocks, LANES), jnp.bfloat16),
            jax.ShapeDtypeStruct((8, LANES), jnp.float32),
        ],
        compiler_params=pltpu.CompilerParams(dimension_semantics=("arbitrary",)),
        cost_estimate=pl.CostEstimate(flops=rows * cols * 8, bytes_accessed=rows * cols * 4, transcendentals=0),
    )(inv, weight)


def flip(m, k):
    bit, out = 1, m
    while bit <= k:
        if k & bit:
            out = out + bit - 2 * bit * ((m // bit) % 2)
        bit *= 2
    return out


def fill_kernel(last, here_ref, own_ref, got_ref, _, out_ref):
    z = here_ref[0]
    end = jnp.logical_and(pl.program_id(0) == 1, jnp.logical_or(z == 0, z == last))

    @pl.when(end)
    def _():
        out_ref[...] = got_ref[...]

    @pl.when(jnp.logical_not(end))
    def _():
        out_ref[...] = own_ref[...]


def fill(out, here, own, got, n, rows, row_block, col_block):
    height, width = own.shape

    def there(step, here):
        z = here[0]
        return jnp.where(step == 0, z, jnp.clip(z, 1, n - 2))

    return pl.pallas_call(
        functools.partial(fill_kernel, n - 1),
        grid_spec=pltpu.PrefetchScalarGridSpec(
            num_scalar_prefetch=1,
            grid=(2,),
            in_specs=[
                pl.BlockSpec((height, width), lambda s, here: (0, 0)),
                pl.BlockSpec((height, width), lambda s, here: (0, 0)),
                pl.BlockSpec(memory_space=pl.ANY),
            ],
            out_specs=pl.BlockSpec(
                (pl.Element(height), pl.Element(width)),
                lambda s, here: (pl.multiple_of(there(s, here) * rows + row_block, 16),
                                 pl.multiple_of(here[1] * width, LANES) if col_block else 0)),
        ),
        out_shape=jax.ShapeDtypeStruct(out.shape, out.dtype),
        input_output_aliases={3: 0},
        compiler_params=pltpu.CompilerParams(dimension_semantics=("arbitrary",)),
        cost_estimate=pl.CostEstimate(flops=0, bytes_accessed=height * width * 8, transcendentals=0),
    )(here, own, got, out)


def copy_kernel(in_ref, out_ref):
    out_ref[...] = in_ref[...]


def copy_all(array, tile):
    rows, cols = array.shape
    spec = pl.BlockSpec((tile, cols), lambda t: (t, 0))
    return pl.pallas_call(
        copy_kernel,
        grid=(rows // tile,),
        in_specs=[spec],
        out_specs=spec,
        out_shape=jax.ShapeDtypeStruct(array.shape, array.dtype),
        compiler_params=pltpu.CompilerParams(dimension_semantics=("arbitrary",)),
        cost_estimate=pl.CostEstimate(flops=0, bytes_accessed=rows * cols * 4, transcendentals=0),
    )(array)


def flip(m, k):
    bit, out = 1, m
    while bit <= k:
        if k & bit:
            out = out + bit - 2 * bit * ((m // bit) % 2)
        bit *= 2
    return out


def move_kernel(n, count, tail, q_ref, s_ref, p_ref, out_ref, tail_ref, so_ref, po_ref,
                a_send, a_recv, z_send, z_recv, own_sem):
    z = lax.axis_index("dp")
    m = lax.axis_index("mp")
    rows, width = q_ref.shape[1:]
    main = rows - tail
    chunk = main // CHUNKS
    order = sorted(range(1, count), key=lambda k: (bin(k).count("1"), k))
    TAIL, SCALE, SUM = CHUNKS, CHUNKS + 1, CHUNKS + 2

    barrier = pltpu.get_barrier_semaphore()
    for k in range(1, count):
        pl.semaphore_signal(barrier, inc=1, device_id=(z, flip(m, k)), device_id_type=MESH)

    @pl.when(z > 0)
    def _():
        pl.semaphore_signal(barrier, inc=1, device_id=(z - 1, m), device_id_type=MESH)

    @pl.when(z < n - 1)
    def _():
        pl.semaphore_signal(barrier, inc=1, device_id=(z + 1, m), device_id_type=MESH)

    beside = jnp.where(z > 0, 1, 0) + jnp.where(z < n - 1, 1, 0)
    pl.semaphore_wait(barrier, count - 1 + beside)

    def span(c):
        return (c * chunk, chunk) if c < CHUNKS else (main, tail)

    def source(c, peer):
        start, size = span(c)
        return q_ref.at[peer, pl.ds(start, size)]

    def columns(src):
        return pl.ds(pl.multiple_of(src * width, LANES), width)

    def place(origin, c, src):
        start, size = span(c)
        return out_ref.at[pl.ds(pl.multiple_of(origin * rows + start, 8), size), columns(src)]

    def landed(c, src):
        if c == TAIL:
            return tail_ref.at[:, columns(src)]
        return place(z, c, src)

    def plane(unit):
        c, k = unit
        peer = flip(m, k)
        if c <= TAIL:
            src, dst = source(c, peer), landed(c, m)
        elif c == SCALE:
            src, dst = s_ref.at[peer], so_ref.at[z, m]
        else:
            src, dst = p_ref, po_ref.at[z, m]
        return pltpu.make_async_remote_copy(
            src_ref=src, dst_ref=dst, send_sem=a_send.at[c, k - 1], recv_sem=a_recv.at[c, k - 1],
            device_id=(z, peer), device_id_type=MESH)

    def ring(unit, way, hop):
        c, k = unit
        origin = z - way * (hop - 1)
        if c <= TAIL:
            dst = place(origin, c, flip(m, k))
            src = dst
            if hop == 1:
                src = source(c, m) if k == 0 else landed(c, flip(m, k))
        else:
            src = dst = (so_ref if c == SCALE else po_ref).at[origin]
        w = 0 if way == 1 else 1
        return pltpu.make_async_remote_copy(
            src_ref=src, dst_ref=dst, send_sem=z_send.at[w, hop - 1, c, k], recv_sem=z_recv.at[w, hop - 1, c, k],
            device_id=(z + way, m), device_id_type=MESH)

    def outside(unit):
        return unit[0] == TAIL or (unit[0] < CHUNKS and unit[1] == 0)

    def sends(unit, way, hop):
        if way == -1:
            able = jnp.logical_and(z > 0, z + hop - 1 <= n - 1)
            return jnp.logical_and(able, z > 1) if hop == 1 and outside(unit) else able
        able = jnp.logical_and(z < n - 1, z - (hop - 1) >= 0)
        return jnp.logical_and(able, z < n - 2) if hop == 1 and outside(unit) else able

    def gets(unit, way, hop):
        if way == -1:
            able = z + hop <= n - 1
            return jnp.logical_and(able, z > 0) if hop == 1 and outside(unit) else able
        able = z - hop >= 0
        return jnp.logical_and(able, z < n - 1) if hop == 1 and outside(unit) else able

    def when(cond, act):
        @pl.when(cond)
        def _():
            act()

    units = [(c, k) for c in range(CHUNKS) for k in [0] + order]
    units = units[:-2] + [(SCALE, 0), (SUM, 0)] + [(TAIL, k) for k in [0] + order] + units[-2:]

    def start_ring(unit):
        for way in (-1, 1):
            when(sends(unit, way, 1), lambda way=way: ring(unit, way, 1).start())

    start_ring((0, 0))
    for k in order:
        plane((0, k)).start()
    for c in range(1, CHUNKS + 1):
        start_ring((c, 0))
    for c in range(1, CHUNKS + 3):
        for k in order:
            plane((c, k)).start()
    owned = {
        TAIL: pltpu.make_async_copy(source(TAIL, m), landed(TAIL, m), own_sem.at[0]),
        SCALE: pltpu.make_async_copy(s_ref.at[m], so_ref.at[z, m], own_sem.at[1]),
        SUM: pltpu.make_async_copy(p_ref, po_ref.at[z, m], own_sem.at[2]),
    }
    for copy in owned.values():
        copy.start()

    for unit in units:
        c, k = unit
        if c <= TAIL and k == 0:
            continue
        if c <= TAIL:
            plane(unit).wait_recv()
        else:
            owned[c].wait()
            for peer in order:
                plane((c, peer)).wait_recv()
        start_ring(unit)

    for hop in range(2, n):
        for unit in units:
            for way in (-1, 1):
                def forward(unit=unit, way=way, hop=hop):
                    ring(unit, way, hop - 1).wait_recv()
                    ring(unit, way, hop).start()

                when(sends(unit, way, hop), forward)

    for hop in range(1, n):
        for unit in units:
            for way in (-1, 1):
                stays = z == 0 if way == -1 else z == n - 1
                when(jnp.logical_and(gets(unit, way, hop), stays),
                     lambda unit=unit, way=way, hop=hop: ring(unit, way, hop).wait_recv())
    owned[TAIL].wait()
    for c in range(CHUNKS + 3):
        for k in order:
            plane((c, k)).wait_send()
    for hop in range(1, n):
        for unit in units:
            for way in (-1, 1):
                when(sends(unit, way, hop),
                     lambda unit=unit, way=way, hop=hop: ring(unit, way, hop).wait_send())


def move(quant, scale, sums, n, tail):
    count, rows, width = quant.shape
    any_spec = pl.BlockSpec(memory_space=pl.ANY)
    dma = pltpu.SemaphoreType.DMA
    sent = rows * width * count * 2 * (n - 1)
    return pl.pallas_call(
        functools.partial(move_kernel, n, count, tail),
        in_specs=[any_spec] * 3,
        out_specs=[any_spec] * 4,
        out_shape=[
            jax.ShapeDtypeStruct((n * rows, count * width), quant.dtype),
            jax.ShapeDtypeStruct((tail, count * width), quant.dtype),
            jax.ShapeDtypeStruct((n, count) + scale.shape[1:], scale.dtype),
            jax.ShapeDtypeStruct((n, count) + sums.shape, sums.dtype),
        ],
        scratch_shapes=[
            dma((CHUNKS + 3, count - 1)),
            dma((CHUNKS + 3, count - 1)),
            dma((2, n - 1, CHUNKS + 3, count)),
            dma((2, n - 1, CHUNKS + 3, count)),
            dma((3,)),
        ],
        compiler_params=pltpu.CompilerParams(collective_id=0, has_side_effects=True),
        cost_estimate=pl.CostEstimate(flops=0, bytes_accessed=sent * 2, transcendentals=0),
    )(quant, scale, sums)


def local(n, weight, rank_map):
    rows, cols = weight.shape
    count = rank_map.shape[0]
    group = cols // LANES // count
    nblocks = count * group
    total_rows = rows * n
    floor = FLOOR_RATIO / math.sqrt(total_rows)
    tail = rows // TAIL_PART
    main = rows - tail
    here = jnp.stack([lax.axis_index("dp"), lax.axis_index("mp")]).astype(jnp.int32)
    ends = [(1, 0), (n - 2, n - 1)]

    head = quantize_head(weight, rank_map, here, floor, main)
    head_got = lax.ppermute(head, "dp", ends)
    quant, scale, sums = quantize(weight, rank_map, floor)
    steps = scale.shape[0]
    scale = scale.reshape(steps, count, group, LANES).transpose(1, 0, 2, 3).reshape(count, steps * group, LANES)
    landed, tail_own, scales, partial_sums = move(quant, scale, sums, n, tail)
    tail_got = lax.ppermute(tail_own, "dp", ends)
    quant_out = copy_all(landed, 2 * LANES)
    quant_out = fill(quant_out, here, head, head_got, n, rows, 0, True)
    quant_out = fill(quant_out, here, tail_own, tail_got, n, rows, main, False)

    scales = scales.reshape(n, count, steps, group, LANES).transpose(0, 2, 4, 1, 3)
    scale_out = scales.reshape(total_rows, nblocks)
    totals = jnp.sum(partial_sums[:, :, 0, :nblocks], axis=0).reshape(-1)
    return (quant_out, scale_out, totals / (127.0 * math.sqrt(total_rows * LANES)))


def solution(mesh):
    n = mesh.shape["dp"]
    in_specs = (P("dp", "mp"), P())
    out_specs = (P(None, "mp"), P(None, "mp"), P())

    def body(weight, rank_map):
        return local(n, weight, rank_map)

    return jax.shard_map(body, mesh=mesh, in_specs=in_specs, out_specs=out_specs, check_vma=False)
```
